32 devices in a mesh: tm: 4 (over y, x), space: 8 (over z, core).
Axes of the slice: x: 2, y: 2, z: 4, core: 2. Of those that a mesh axis runs over, the one named last changes fastest.
Arguments:
- residual: float32 [64, 64, 8, 128], P('tm', 'space'), may hold values from -24 to 24
- capacity: float32 [64, 8, 128], P('space'), may hold values from 0.25 to 4
Outputs:
- preconditioned: float32 [64, 64, 8, 128], P('tm', 'space')
The draws below stay inside these ranges and needn't reach their ends.
All inputs are finite; a program needn't handle non-finite values.
Results may differ from the reference program's by a relative error of at most 0.0003.
Values sent between devices are 32-bit elements; how exact they have to be, the bound alone decides.
No kernel may reach another device: no remote copies, remote signals or barrier semaphores. Data moves between devices by JAX's collectives and lax.ppermute only.
A program may use at most 64 MiB of HBM per device.

```python
import math
import jax
import jax.numpy as jnp
from jax import lax

NY = 8
NZ = 128
TSTEPS = 64
GRID_DEPTH = 4
SMOOTH = 2
COARSE_SWEEPS = 6
NX = 64


def draw_residual(key, part):
    extents = (TSTEPS, NX, NY, NZ)
    return jnp.clip(4.0 * jax.random.normal(jax.random.fold_in(key, 11), extents, jnp.float32), -24.0, 24.0)


def levels(stream_key, shape, shards, smallest, high):
    loudness = 1.0
    for dim, parts in shards:
        steps = jax.random.uniform(jax.random.fold_in(jax.random.fold_in(stream_key, 6), dim), (parts,), jnp.float32, smallest / len(shards), high / len(shards))
        loudness = loudness * jnp.repeat(jnp.exp(steps), shape[dim] // parts).reshape((-1,) + (1,) * (len(shape) - 1 - dim))
    return loudness


def setup_inputs(seed: int = 0) -> dict:
    arg_keys = jax.random.split(jax.random.key(seed), 3)
    return {
        "residual": draw_residual(jax.random.fold_in(arg_keys[2], 71), 0),
        "capacity": jnp.clip(jnp.exp(math.log(4.0) - 2.7725887 * jax.random.uniform(arg_keys[1], (NX, NY, NZ), jnp.float32) ** levels(arg_keys[1], (NX, NY, NZ), ((0, 8),), -0.2, 0.2)), 0.25, 4.0),
    }


ALPHA_CORNER = 0.01
STEP_SIZE = 0.5
DIFFUSE = 2.0
ADVECT = (0.2, -0.15, 0.1)
OMEGA = 0.7
HIGHEST = lax.Precision.HIGHEST


def level_coefficients(per_level_values):
    spread = DIFFUSE / 4.0 ** per_level_values
    drifts = tuple(component / 2.0 ** per_level_values for component in ADVECT)
    return spread, drifts


def pad_second(volume, position):
    widths = [(0, 0)] * volume.ndim
    widths[position] = (1, 1)
    return jnp.pad(volume, widths)


def apply_operator(padded, current_capacity, spectral_shifts, per_level_values):
    spread, drifts = level_coefficients(per_level_values)
    centre = padded[:, :, 1:-1]
    upper_first = padded[:, :, 2:]
    lower_first = padded[:, :, :-2]
    wide_second = pad_second(centre, 3)
    upper_second = wide_second[:, :, :, 2:]
    lower_second = wide_second[:, :, :, :-2]
    wide_third = pad_second(centre, 4)
    upper_third = wide_third[:, :, :, :, 2:]
    lower_third = wide_third[:, :, :, :, :-2]
    stencil = spread * (6.0 * centre - upper_first - lower_first - upper_second - lower_second - upper_third - lower_third)
    stencil = stencil + drifts[0] * (upper_first - lower_first) + drifts[1] * (upper_second - lower_second) + drifts[2] * (upper_third - lower_third)
    first_shift, second_shift, third_shift = spectral_shifts
    real_part = centre[0]
    imag_part = centre[1]
    shifted = jnp.stack([current_capacity * (first_shift * real_part - second_shift * imag_part), current_capacity * (second_shift * real_part + third_shift * imag_part)])
    return stencil + shifted


def inverse_diagonal(current_capacity, spectral_shifts, per_level_values):
    spread, drifts = level_coefficients(per_level_values)
    first_shift, second_shift, third_shift = spectral_shifts
    top_left = current_capacity * first_shift + 6.0 * spread
    coupling = current_capacity * second_shift
    bottom_right = current_capacity * third_shift + 6.0 * spread
    determinant = top_left * bottom_right + coupling * coupling
    return bottom_right / determinant, coupling / determinant, top_left / determinant


def damped_update(residual_now, inverse):
    diagonal_a, diagonal_b, diagonal_c = inverse
    return OMEGA * jnp.stack([diagonal_a * residual_now[0] + diagonal_b * residual_now[1], diagonal_c * residual_now[1] - diagonal_b * residual_now[0]])


def restrict_to_coarse(volume):
    leading = volume.shape[:-3]
    first_extent, second_extent, third_extent = volume.shape[-3:]
    blocks = volume.reshape(leading + (first_extent // 2, 2, second_extent // 2, 2, third_extent // 2, 2))
    lead_count = len(leading)
    return jnp.mean(blocks, axis=(lead_count + 1, lead_count + 3, lead_count + 5))


def prolong_cells(volume):
    leading = volume.shape[:-3]
    first_extent, second_extent, third_extent = volume.shape[-3:]
    expanded = jnp.broadcast_to(volume[..., :, None, :, None, :, None], leading + (first_extent, 2, second_extent, 2, third_extent, 2))
    return expanded.reshape(leading + (2 * first_extent, 2 * second_extent, 2 * third_extent))


def shift_values(frequency, length):
    ratio_step = ALPHA_CORNER ** (1.0 / length)
    phases = (2.0 * math.pi / length) * frequency.astype(jnp.float32)
    first_shift = (1.0 - ratio_step * jnp.cos(phases)) / STEP_SIZE
    second_shift = ratio_step * jnp.sin(phases) / STEP_SIZE
    return tuple(column.reshape(-1, 1, 1, 1) for column in (first_shift, second_shift, first_shift))


def multigrid_cycle(per_level_values, forcing_term, capacity_fields, spectral_shifts):
    current_capacity = capacity_fields[per_level_values]
    inverse = inverse_diagonal(current_capacity, spectral_shifts, per_level_values)
    coarsest = per_level_values == GRID_DEPTH - 1
    current = damped_update(forcing_term, inverse)
    for repeat in range((COARSE_SWEEPS if coarsest else SMOOTH) - 1):
        current = current + damped_update(forcing_term - apply_operator(pad_second(current, 2), current_capacity, spectral_shifts, per_level_values), inverse)
    if coarsest:
        return current
    coarse_right_hand = restrict_to_coarse(forcing_term - apply_operator(pad_second(current, 2), current_capacity, spectral_shifts, per_level_values))
    coarse_solution = multigrid_cycle(per_level_values + 1, coarse_right_hand, capacity_fields, spectral_shifts)
    current = current + prolong_cells(coarse_solution)
    for repeat in range(SMOOTH):
        current = current + damped_update(forcing_term - apply_operator(pad_second(current, 2), current_capacity, spectral_shifts, per_level_values), inverse)
    return current


def reference(residual, capacity):
    length = residual.shape[0]
    ratio_step = ALPHA_CORNER ** (1.0 / length)
    moments = jnp.arange(length, dtype=jnp.float32)
    weights = jnp.power(ratio_step, moments)
    scaled = residual * weights[:, None, None, None]
    capacity_fields = [capacity]
    for per_level_values in range(1, GRID_DEPTH):
        capacity_fields.append(restrict_to_coarse(capacity_fields[-1]))
    integers = jnp.arange(length, dtype=jnp.int32)

    def one_frequency(summed, frequency):
        phases = (2.0 * math.pi / length) * ((integers * frequency) % length).astype(jnp.float32)
        cosines = jnp.cos(phases)
        sines = jnp.sin(phases)
        real_part = jnp.tensordot(cosines, scaled, axes=1, precision=HIGHEST)
        imag_part = -jnp.tensordot(sines, scaled, axes=1, precision=HIGHEST)
        forcing_term = jnp.stack([real_part, imag_part])[:, None]
        spectral_shifts = shift_values(frequency[None], length)
        solution_field = multigrid_cycle(0, forcing_term, capacity_fields, spectral_shifts)[:, 0]
        summed = summed + cosines[:, None, None, None] * solution_field[0] - sines[:, None, None, None] * solution_field[1]
        return summed, None

    summed, unused = lax.scan(one_frequency, jnp.zeros(residual.shape, jnp.float32), integers)
    return summed / length / weights[:, None, None, None]
```

```python
import functools
import math

import jax
import jax.numpy as jnp
from jax import lax
from jax.experimental import pallas as pl
from jax.experimental.pallas import tpu as pltpu
from jax.sharding import PartitionSpec as P

GRID_DEPTH = 4
SMOOTH = 2
COARSE_SWEEPS = 6


ALPHA_CORNER = 0.01
STEP_SIZE = 0.5
DIFFUSE = 2.0
ADVECT = (0.2, -0.15, 0.1)
OMEGA = 0.7
HIGHEST = lax.Precision.HIGHEST


def extended(array, sides, width):
    for axis, dim in sides:
        peers, length = (lax.axis_size(axis), array.shape[dim])
        up = [(i, (i + 1) % peers) for i in range(peers - 1)]
        down = [(j, i) for i, j in up]
        last = lax.slice_in_dim(array, length - width, length, axis=dim)
        initial = lax.slice_in_dim(array, 0, width, axis=dim)
        before = lax.ppermute(last, axis, up)
        after = lax.ppermute(initial, axis, down)
        array = jnp.concatenate([before, array, after], axis=dim)
    return array


def level_coefficients(per_level_values):
    spread = DIFFUSE / 4.0**per_level_values
    drifts = tuple((component / 2.0**per_level_values for component in ADVECT))
    return (spread, drifts)


def pad_second(volume, position):
    widths = [(0, 0)] * volume.ndim
    widths[position] = (1, 1)
    return jnp.pad(volume, widths)


def apply_operator(padded, current_capacity, spectral_shifts, per_level_values):
    spread, drifts = level_coefficients(per_level_values)
    centre = padded[:, :, 1:-1]
    upper_first = padded[:, :, 2:]
    lower_first = padded[:, :, :-2]
    wide_second = pad_second(centre, 3)
    upper_second = wide_second[:, :, :, 2:]
    lower_second = wide_second[:, :, :, :-2]
    wide_third = pad_second(centre, 4)
    upper_third = wide_third[:, :, :, :, 2:]
    lower_third = wide_third[:, :, :, :, :-2]
    stencil = spread * (
        6.0 * centre
        - upper_first
        - lower_first
        - upper_second
        - lower_second
        - upper_third
        - lower_third
    )
    stencil = (
        stencil
        + drifts[0] * (upper_first - lower_first)
        + drifts[1] * (upper_second - lower_second)
        + drifts[2] * (upper_third - lower_third)
    )
    first_shift, second_shift, third_shift = spectral_shifts
    real_part = centre[0]
    imag_part = centre[1]
    shifted = jnp.stack(
        [
            current_capacity * (first_shift * real_part - second_shift * imag_part),
            current_capacity * (second_shift * real_part + third_shift * imag_part),
        ]
    )
    return stencil + shifted


def inverse_diagonal(current_capacity, spectral_shifts, per_level_values):
    spread, drifts = level_coefficients(per_level_values)
    first_shift, second_shift, third_shift = spectral_shifts
    top_left = current_capacity * first_shift + 6.0 * spread
    coupling = current_capacity * second_shift
    bottom_right = current_capacity * third_shift + 6.0 * spread
    determinant = top_left * bottom_right + coupling * coupling
    return (bottom_right / determinant, coupling / determinant, top_left / determinant)


def damped_update(residual_now, inverse):
    diagonal_a, diagonal_b, diagonal_c = inverse
    return OMEGA * jnp.stack(
        [
            diagonal_a * residual_now[0] + diagonal_b * residual_now[1],
            diagonal_c * residual_now[1] - diagonal_b * residual_now[0],
        ]
    )


def restrict_to_coarse(volume):
    leading = volume.shape[:-3]
    first_extent, second_extent, third_extent = volume.shape[-3:]
    blocks = volume.reshape(
        leading + (first_extent // 2, 2, second_extent // 2, 2, third_extent // 2, 2)
    )
    lead_count = len(leading)
    return jnp.mean(blocks, axis=(lead_count + 1, lead_count + 3, lead_count + 5))


def prolong_cells(volume):
    leading = volume.shape[:-3]
    first_extent, second_extent, third_extent = volume.shape[-3:]
    expanded = jnp.broadcast_to(
        volume[..., :, None, :, None, :, None],
        leading + (first_extent, 2, second_extent, 2, third_extent, 2),
    )
    return expanded.reshape(leading + (2 * first_extent, 2 * second_extent, 2 * third_extent))


def shift_values(frequency, length):
    ratio_step = ALPHA_CORNER ** (1.0 / length)
    phases = 2.0 * math.pi / length * frequency.astype(jnp.float32)
    first_shift = (1.0 - ratio_step * jnp.cos(phases)) / STEP_SIZE
    second_shift = ratio_step * jnp.sin(phases) / STEP_SIZE
    leading = frequency == 0
    second_shift = jnp.where(leading, 0.0, second_shift)
    third_shift = jnp.where(leading, (1.0 + ratio_step) / STEP_SIZE, first_shift)
    return tuple(
        (column.reshape(-1, 1, 1, 1) for column in (first_shift, second_shift, third_shift))
    )


def phase_grid(row_count, length):
    integers = (
        jnp.arange(row_count, dtype=jnp.int32)[:, None]
        * jnp.arange(length, dtype=jnp.int32)[None, :]
        % length
    )
    return 2.0 * math.pi / length * integers.astype(jnp.float32)


def pad_faces(volume):
    return extended(volume, (("space", 2),), 1)


def multigrid_cycle(
    per_level_values,
    forcing_term,
    capacity_fields,
    spectral_shifts,
    shared_values,
    assemble_level,
    assemble_parts,
):
    current_capacity = capacity_fields[per_level_values]
    inverse = inverse_diagonal(current_capacity, spectral_shifts, per_level_values)
    coarsest = per_level_values == GRID_DEPTH - 1
    current = damped_update(forcing_term, inverse)
    for repeat in range((COARSE_SWEEPS if coarsest else SMOOTH) - 1):
        current = current + damped_update(
            forcing_term
            - apply_operator(
                pad_faces(current), current_capacity, spectral_shifts, per_level_values
            ),
            inverse,
        )
    if coarsest:
        return current
    coarse_right_hand = restrict_to_coarse(
        forcing_term
        - apply_operator(pad_faces(current), current_capacity, spectral_shifts, per_level_values)
    )
    coarse_solution = multigrid_cycle(
        per_level_values + 1,
        coarse_right_hand,
        capacity_fields,
        spectral_shifts,
        shared_values,
        assemble_level,
        assemble_parts,
    )
    current = current + prolong_cells(coarse_solution)
    for repeat in range(SMOOTH):
        current = current + damped_update(
            forcing_term
            - apply_operator(
                pad_faces(current), current_capacity, spectral_shifts, per_level_values
            ),
            inverse,
        )
    return current


def slab_program(residual, capacity):
    steps_here, thickness, extent_second, extent_third = residual.shape
    length = lax.axis_size("tm") * steps_here
    ratio_step = ALPHA_CORNER ** (1.0 / length)
    moments = (lax.axis_index("tm") * steps_here + jnp.arange(steps_here, dtype=jnp.int32)).astype(
        jnp.float32
    )
    scaled = (residual * jnp.power(ratio_step, moments)[:, None, None, None]).reshape(
        steps_here, -1
    )
    series = lax.all_to_all(scaled, "tm", split_axis=1, concat_axis=0, tiled=True)
    all_weights = jnp.power(ratio_step, jnp.arange(length, dtype=jnp.float32))
    alternate = 1.0 - 2.0 * (jnp.arange(length, dtype=jnp.int32) % 2).astype(jnp.float32)
    capacity_fields = [capacity]
    for per_level_values in range(1, GRID_DEPTH):
        capacity_fields.append(restrict_to_coarse(capacity_fields[-1]))
    halves = length // 2
    phases = phase_grid(halves, length)
    first_row = jnp.arange(halves, dtype=jnp.int32)[:, None] == 0
    forward = jnp.concatenate(
        [jnp.cos(phases), jnp.where(first_row, alternate[None, :], -jnp.sin(phases))], axis=0
    )
    spectrum = jnp.dot(forward, series, precision=HIGHEST).reshape(2, halves, -1)
    received = lax.all_to_all(spectrum, "tm", split_axis=1, concat_axis=2, tiled=True)
    slot_count = steps_here // 2
    frequency = lax.axis_index("tm") * slot_count + jnp.arange(slot_count, dtype=jnp.int32)
    spectral_shifts = shift_values(frequency, length)
    field_list = received.reshape(2, slot_count, thickness, extent_second, extent_third)
    solved_fields = multigrid_cycle(
        0, field_list, capacity_fields, spectral_shifts, False, GRID_DEPTH, None
    )
    flattened = solved_fields.reshape(2, slot_count, -1)
    returned = lax.all_to_all(flattened, "tm", split_axis=2, concat_axis=1, tiled=True)
    halves = length // 2
    phases = jnp.transpose(phase_grid(halves, length))
    first_column = jnp.arange(halves, dtype=jnp.int32)[None, :] == 0
    real_columns = jnp.where(first_column, 1.0, 2.0 * jnp.cos(phases)) / length
    imag_columns = jnp.where(first_column, alternate[:, None], -2.0 * jnp.sin(phases)) / length
    inverse_table = jnp.concatenate([real_columns, imag_columns], axis=1)
    values = jnp.dot(
        inverse_table,
        returned.reshape(returned.shape[0] * returned.shape[1], -1),
        precision=HIGHEST,
    )
    values = values / all_weights[:, None]
    result = lax.all_to_all(values, "tm", split_axis=0, concat_axis=1, tiled=True)
    return result.reshape(residual.shape)


def complex_add(p, q):
    return (p[0] + q[0], p[1] + q[1])


def complex_sub(p, q):
    return (p[0] - q[0], p[1] - q[1])


def complex_scale(p, cosine, sine):
    real, imag = p
    if abs(sine) < 1e-12:
        if abs(cosine - 1.0) < 1e-12:
            return p
        return (cosine * real, None if imag is None else cosine * imag)
    if imag is None:
        return (None if abs(cosine) < 1e-12 else cosine * real, sine * real)
    if abs(cosine) < 1e-12:
        if abs(sine - 1.0) < 1e-12:
            return (-imag, real)
        if abs(sine + 1.0) < 1e-12:
            return (imag, -real)
        return (-sine * imag, sine * real)
    return (cosine * real - sine * imag, cosine * imag + sine * real)


def full(p, like):
    return tuple(jnp.zeros_like(like) if part is None else part for part in p)


def transform(points, sign):
    count = len(points)
    if count == 1:
        return points
    if count % 2:
        sums = []
        for m in range(count):
            total = points[0]
            for s in range(1, count):
                angle = sign * 2.0 * math.pi * ((m * s) % count) / count
                term = complex_scale(points[s], math.cos(angle), math.sin(angle))
                total = complex_add(total, term)
            sums.append(total)
        return sums
    even = transform(points[0::2], sign)
    odd = transform(points[1::2], sign)
    low, high = [], []
    for m in range(count // 2):
        angle = sign * 2.0 * math.pi * m / count
        turned = complex_scale(odd[m], math.cos(angle), math.sin(angle))
        low.append(complex_add(even[m], turned))
        high.append(complex_sub(even[m], turned))
    return low + high


def pick(index, values):
    chosen = jnp.float32(values[-1])
    for place in range(len(values) - 1):
        chosen = jnp.where(index == place, jnp.float32(values[place]), chosen)
    return chosen


def forward_kernel(*refs):
    chunks, out = refs[:4], refs[4]
    steps, planes = chunks[0].shape[:2]
    length = 4 * steps
    ratio = ALPHA_CORNER ** (1.0 / length)
    me = lax.axis_index("tm")
    weights = []
    for m in range(4):
        block = jnp.bitwise_xor(me, m)
        grow = [ratio ** (steps * d) for d in range(4)]
        weights.append(
            (
                pick(block, grow),
                pick(block, [grow[0], -grow[1], grow[2], -grow[3]]),
                pick(block, [grow[0], 0.0, -grow[2], 0.0]),
                pick(block, [0.0, -grow[1], 0.0, grow[3]]),
            )
        )

    def column(j, carry):
        sums = [[], [], [], []]
        for s in range(steps):
            values = [chunk[s, j] for chunk in chunks]
            for kind in range(4):
                total = weights[0][kind] * values[0]
                for m in range(1, 4):
                    total = total + weights[m][kind] * values[m]
                sums[kind].append(total)

        def turned(real, imag, remainder):
            points = []
            for s in range(steps):
                angle = -2.0 * math.pi * remainder * s / length
                size = ratio**s
                point = (real[s], None if imag is None else imag[s])
                point = complex_scale(point, size * math.cos(angle), size * math.sin(angle))
                points.append(full(point, real[s]))
            return transform(points, -1.0)

        halves = length // 2
        found = {}
        for remainder, real, imag in ((0, sums[0], None), (2, sums[1], None), (1, sums[2], sums[3])):
            for m, value in enumerate(turned(real, imag, remainder)):
                slot = 4 * m + remainder
                if slot <= halves:
                    found[slot] = value
                elif remainder == 1:
                    found[length - slot] = (value[0], -value[1])
        out[0, 0, j] = found[0][0]
        out[0, 1, j] = found[halves][0]
        for slot in range(1, halves):
            out[slot, 0, j] = found[slot][0]
            out[slot, 1, j] = found[slot][1]
        return carry

    lax.fori_loop(0, planes, column, 0)


def backward_kernel(spectrum, *outs):
    steps, planes = outs[0].shape[:2]
    length = 4 * steps
    halves = length // 2
    ratio = ALPHA_CORNER ** (1.0 / length)
    me = lax.axis_index("tm")
    weights = []
    for m in range(4):
        block = jnp.bitwise_xor(me, m)
        grow = [ratio ** (-steps * d) / length for d in range(4)]
        weights.append(
            (
                pick(block, grow),
                pick(block, [grow[0], -grow[1], grow[2], -grow[3]]),
                pick(block, [2.0 * grow[0], 0.0, -2.0 * grow[2], 0.0]),
                pick(block, [0.0, -2.0 * grow[1], 0.0, 2.0 * grow[3]]),
            )
        )

    def column(j, carry):
        def value(slot):
            if slot == 0:
                return (spectrum[0, 0, j], jnp.zeros_like(spectrum[0, 0, j]))
            if slot == halves:
                return (spectrum[0, 1, j], jnp.zeros_like(spectrum[0, 1, j]))
            if slot < halves:
                return (spectrum[slot, 0, j], spectrum[slot, 1, j])
            return (spectrum[length - slot, 0, j], -spectrum[length - slot, 1, j])

        def turned(remainder):
            points = transform([value(4 * m + remainder) for m in range(steps)], 1.0)
            result = []
            for s in range(steps):
                angle = 2.0 * math.pi * remainder * s / length
                size = ratio**-s
                result.append(
                    complex_scale(points[s], size * math.cos(angle), size * math.sin(angle))
                )
            return result

        zero, two, one = turned(0), turned(2), turned(1)
        for s in range(steps):
            parts = (zero[s][0], two[s][0], one[s][0], one[s][1])
            for m in range(4):
                total = weights[m][0] * parts[0]
                for kind in range(1, 4):
                    total = total + weights[m][kind] * parts[kind]
                outs[m][s, j] = total
        return carry

    lax.fori_loop(0, planes, column, 0)


def place_kernel(*refs):
    chunks, out = refs[:4], refs[4]
    steps, planes = chunks[0].shape[:2]
    me = lax.axis_index("tm")

    def one_step(s, carry):
        for m in range(4):
            block = jnp.bitwise_xor(me, m)
            for j in range(planes):
                out[s, block * planes + j] = chunks[m][s, j]
        return carry

    lax.fori_loop(0, steps, one_step, 0, unroll=4)


def cycle_kernel(blocks, forcing, out, *scratch, tm_count, space_count, order):
    rows, lanes = forcing.shape[-2:]
    planes = forcing.shape[2]
    thickness = blocks.shape[1]
    slots = forcing.shape[0]
    length = 2 * slots
    ratio = ALPHA_CORNER ** (1.0 / length)
    me_space = lax.axis_index("space")
    slot = lax.axis_index("tm") * space_count + me_space
    angles = [2.0 * math.pi * k / length for k in range(slots)]
    first = [(1.0 - ratio * math.cos(a)) / STEP_SIZE for a in angles]
    second = [ratio * math.sin(a) / STEP_SIZE for a in angles]
    third = list(first)
    second[0] = 0.0
    third[0] = (1.0 + ratio) / STEP_SIZE
    first, second, third = (pick(slot, values) for values in (first, second, third))

    fields = [
        dict(zip(("capacity", "a", "b", "c", "u", "w", "g"), scratch[7 * l : 7 * l + 7]))
        for l in range(GRID_DEPTH)
    ]
    row = lax.broadcasted_iota(jnp.int32, (rows, lanes), 0)
    lane = lax.broadcasted_iota(jnp.int32, (rows, lanes), 1)

    for block, distance in enumerate(order):
        target = jnp.bitwise_xor(me_space, distance) * thickness
        for x in range(thickness):
            fields[0]["capacity"][target + x] = blocks[block, x]

    def loop(count, group, body):
        if count <= group:
            for p in range(count):
                body(0, p)
        else:
            assert count % group == 0

            def step(i, carry):
                base = i * group
                for p in range(group):
                    body(base, p)
                return carry

            lax.fori_loop(0, count // group, step, 0)

    def pair_sum(value, level):
        stride = 2**level
        if stride < rows:
            bit = (row // stride) % 2 == 1
            value = value + jnp.where(
                bit, pltpu.roll(value, stride, 0), pltpu.roll(value, rows - stride, 0)
            )
        bit = (lane // stride) % 2 == 1
        return value + jnp.where(
            bit, pltpu.roll(value, stride, 1), pltpu.roll(value, lanes - stride, 1)
        )

    def level_count(level):
        return fields[level]["capacity"].shape[0]

    for level in range(1, GRID_DEPTH):
        fine, coarse = fields[level - 1]["capacity"], fields[level]["capacity"]

        def shrink(base, p, fine=fine, coarse=coarse, level=level):
            pair = fine[2 * (base + p)] + fine[2 * (base + p) + 1]
            coarse[base + p] = 0.125 * pair_sum(pair, level - 1)

        loop(level_count(level), 8, shrink)

    def stencil(level):
        spread, drifts = level_coefficients(level)
        stride = 2**level
        extents = (rows // stride, lanes // stride)
        cell = (row // stride, lane // stride)
        masks = []
        for d in range(2):
            up = jnp.where(cell[d] < extents[d] - 1, spread - drifts[d + 1], 0.0)
            down = jnp.where(cell[d] > 0, spread + drifts[d + 1], 0.0)
            masks.append((up, down))

        def apply(here, up, down):
            total = (spread - drifts[0]) * up + (spread + drifts[0]) * down
            if extents[0] > 1:
                total = total + masks[0][0] * pltpu.roll(here, rows - stride, 0)
                total = total + masks[0][1] * pltpu.roll(here, stride, 0)
            total = total + masks[1][0] * pltpu.roll(here, lanes - stride, 1)
            return total + masks[1][1] * pltpu.roll(here, stride, 1)

        return apply

    def forcing_at(level, group, base, p):
        if level:
            ref = fields[level]["g"]
            return ref[base + p, 0], ref[base + p, 1]
        source, inner = base // thickness, p
        index = (inner // planes) * space_count + source
        return forcing[index, 0, inner % planes], forcing[index, 1, inner % planes]

    def start(level):
        field = fields[level]
        spread, _ = level_coefficients(level)
        zero = jnp.zeros((rows, lanes), jnp.float32)
        for name in ("u", "w"):
            for edge in (0, level_count(level) + 1):
                field[name][edge, 0] = zero
                field[name][edge, 1] = zero

        def body(base, p):
            here = base + p
            size = field["capacity"][here]
            top = size * first + 6.0 * spread
            couple = size * second
            bottom = size * third + 6.0 * spread
            inverse = OMEGA / (top * bottom + couple * couple)
            a, b, c = bottom * inverse, couple * inverse, top * inverse
            field["a"][here] = a
            field["b"][here] = b
            field["c"][here] = c
            real, imag = forcing_at(level, group_of(level), base, p)
            field["u"][here + 1, 0] = a * real + b * imag
            field["u"][here + 1, 1] = c * imag - b * real

        loop(level_count(level), group_of(level), body)

    def group_of(level):
        return thickness

    def right_side(level, apply, source, base, p):
        here = base + p
        real, imag = forcing_at(level, group_of(level), base, p)
        v_real, v_imag = source[here + 1, 0], source[here + 1, 1]
        r_real = real + apply(v_real, source[here + 2, 0], source[here, 0])
        r_imag = imag + apply(v_imag, source[here + 2, 1], source[here, 1])
        return v_real, v_imag, r_real, r_imag

    def sweep(level, source, store):
        field, apply = fields[level], stencil(level)

        def body(base, p):
            here = base + p
            v_real, v_imag, r_real, r_imag = right_side(level, apply, source, base, p)
            a, b, c = field["a"][here], field["b"][here], field["c"][here]
            new_real = (1.0 - OMEGA) * v_real + (a * r_real + b * r_imag)
            new_imag = (1.0 - OMEGA) * v_imag + (c * r_imag - b * r_real)
            store(base, p, new_real, new_imag)

        loop(level_count(level), group_of(level), body)

    def storing(ref):
        def store(base, p, real, imag):
            ref[base + p + 1, 0] = real
            ref[base + p + 1, 1] = imag

        return store

    def store_out(base, p, real, imag):
        index = (p // planes) * space_count + base // thickness
        out[index, 0, p % planes] = real
        out[index, 1, p % planes] = imag

    def descend(level, source):
        field, apply = fields[level], stencil(level)
        spread, _ = level_coefficients(level)
        coarse = fields[level + 1]["g"]

        def defect(base, p):
            here = base + p
            v_real, v_imag, r_real, r_imag = right_side(level, apply, source, base, p)
            size = field["capacity"][here]
            real = r_real - 6.0 * spread * v_real - size * (first * v_real - second * v_imag)
            imag = r_imag - 6.0 * spread * v_imag - size * (second * v_real + third * v_imag)
            return real, imag

        def body(base, p):
            if p % 2:
                return
            low, high = defect(base, p), defect(base, p + 1)
            target = (base + p) // 2
            for part in range(2):
                coarse[target, part] = 0.125 * pair_sum(low[part] + high[part], level)

        loop(level_count(level), group_of(level), body)

    def cycle(level, last_store):
        field = fields[level]
        here, other = field["u"], field["w"]
        start(level)
        coarsest = level == GRID_DEPTH - 1
        for repeat in range((COARSE_SWEEPS if coarsest else SMOOTH) - 1):
            sweep(level, here, storing(other))
            here, other = other, here
        if coarsest:
            return here
        descend(level, here)
        value = cycle(level + 1, None)

        def correct(base, p, here=here):
            at = base + p
            for part in range(2):
                here[at + 1, part] = here[at + 1, part] + value[at // 2 + 1, part]

        loop(level_count(level), group_of(level), correct)
        for repeat in range(SMOOTH):
            final = repeat == SMOOTH - 1 and last_store is not None
            sweep(level, here, last_store if final else storing(other))
            here, other = other, here
        return here

    cycle(0, store_out)


def call(kernel, shapes, *operands, scratch=()):
    return pl.pallas_call(
        kernel,
        out_shape=shapes,
        in_specs=[pl.BlockSpec(memory_space=pltpu.VMEM)] * len(operands),
        out_specs=jax.tree.map(lambda s: pl.BlockSpec(memory_space=pltpu.VMEM), shapes),
        scratch_shapes=scratch,
    )(*operands)


def gather_capacity(capacity, space_count):
    blocks, strides = capacity[None], []
    order = [0]
    stride = 2
    while stride < space_count:
        strides.append(stride)
        stride *= 2
    strides.append(1)
    for stride in strides:
        pairs = [(k, k ^ stride) for k in range(space_count)]
        blocks = jnp.concatenate([blocks, lax.ppermute(blocks, "space", pairs)], axis=0)
        order = order + [place ^ stride for place in order]
    return blocks, order


def slot_program(residual, capacity):
    steps, thickness, rows, lanes = residual.shape
    tm_count, space_count = lax.axis_size("tm"), lax.axis_size("space")
    slots = tm_count * space_count
    planes = thickness // tm_count
    me = lax.axis_index("tm")
    split = residual.reshape(steps, tm_count, planes, rows, lanes)
    chunks = []
    for m in range(tm_count):
        chunks.append(
            lax.dynamic_index_in_dim(split, jnp.bitwise_xor(me, m), axis=1, keepdims=False)
        )
    swaps = [[(k, k ^ m) for k in range(tm_count)] for m in range(tm_count)]
    for m in range(1, tm_count):
        chunks[m] = lax.ppermute(chunks[m], "tm", swaps[m])
    blocks, order = gather_capacity(capacity, space_count)
    spectrum = call(
        forward_kernel,
        jax.ShapeDtypeStruct((slots, 2, planes, rows, lanes), jnp.float32),
        *chunks,
    )
    spectrum = lax.all_to_all(spectrum, ("tm", "space"), 0, 0, tiled=True)
    scratch = []
    for level in range(GRID_DEPTH):
        count = (thickness * space_count) >> level
        scratch += [pltpu.VMEM((count, rows, lanes), jnp.float32)] * 4
        scratch += [pltpu.VMEM((count + 2, 2, rows, lanes), jnp.float32)] * 2
        small = level == 0
        scratch += [pltpu.VMEM((1 if small else count, 2, rows, lanes), jnp.float32)]
    solved = call(
        functools.partial(
            cycle_kernel, tm_count=tm_count, space_count=space_count, order=tuple(order)
        ),
        jax.ShapeDtypeStruct(spectrum.shape, jnp.float32),
        blocks,
        spectrum,
        scratch=scratch,
    )
    solved = lax.all_to_all(solved, ("tm", "space"), 0, 0, tiled=True)
    chunk = jax.ShapeDtypeStruct((steps, planes, rows, lanes), jnp.float32)
    pieces = list(call(backward_kernel, (chunk,) * tm_count, solved))
    for m in range(1, tm_count):
        pieces[m] = lax.ppermute(pieces[m], "tm", swaps[m])
    return call(place_kernel, jax.ShapeDtypeStruct(residual.shape, jnp.float32), *pieces)


def on_device(residual, capacity):
    steps, thickness, rows, lanes = residual.shape
    tm_count, space_count = lax.axis_size("tm"), lax.axis_size("space")
    whole = (
        tm_count == 4
        and 2 * space_count == steps
        and space_count & (space_count - 1) == 0
        and space_count > 1
        and thickness % tm_count == 0
        and thickness % 2 == 0
    )
    if whole:
        return slot_program(residual, capacity)
    return slab_program(residual, capacity)


def solution(mesh):
    return jax.shard_map(
        on_device,
        mesh=mesh,
        in_specs=(P("tm", "space", None, None), P("space", None, None)),
        out_specs=P("tm", "space", None, None),
        check_vma=False,
    )
```

```python
import functools
import math

import jax
import jax.numpy as jnp
from jax import lax
from jax.experimental import pallas as pl
from jax.experimental.pallas import tpu as pltpu
from jax.sharding import PartitionSpec as P

GRID_DEPTH = 4
SMOOTH = 2
COARSE_SWEEPS = 6


ALPHA_CORNER = 0.01
STEP_SIZE = 0.5
DIFFUSE = 2.0
ADVECT = (0.2, -0.15, 0.1)
OMEGA = 0.7
HIGHEST = lax.Precision.HIGHEST
VMEM_LIMIT = 16 * 2**20
GROUP = 2


def extended(array, sides, width):
    for axis, dim in sides:
        peers, length = (lax.axis_size(axis), array.shape[dim])
        up = [(i, (i + 1) % peers) for i in range(peers - 1)]
        down = [(j, i) for i, j in up]
        last = lax.slice_in_dim(array, length - width, length, axis=dim)
        initial = lax.slice_in_dim(array, 0, width, axis=dim)
        before = lax.ppermute(last, axis, up)
        after = lax.ppermute(initial, axis, down)
        array = jnp.concatenate([before, array, after], axis=dim)
    return array


def level_coefficients(per_level_values):
    spread = DIFFUSE / 4.0**per_level_values
    drifts = tuple((component / 2.0**per_level_values for component in ADVECT))
    return (spread, drifts)


def pad_second(volume, position):
    widths = [(0, 0)] * volume.ndim
    widths[position] = (1, 1)
    return jnp.pad(volume, widths)


def apply_operator(padded, current_capacity, spectral_shifts, per_level_values):
    spread, drifts = level_coefficients(per_level_values)
    centre = padded[:, :, 1:-1]
    upper_first = padded[:, :, 2:]
    lower_first = padded[:, :, :-2]
    wide_second = pad_second(centre, 3)
    upper_second = wide_second[:, :, :, 2:]
    lower_second = wide_second[:, :, :, :-2]
    wide_third = pad_second(centre, 4)
    upper_third = wide_third[:, :, :, :, 2:]
    lower_third = wide_third[:, :, :, :, :-2]
    stencil = spread * (
        6.0 * centre
        - upper_first
        - lower_first
        - upper_second
        - lower_second
        - upper_third
        - lower_third
    )
    stencil = (
        stencil
        + drifts[0] * (upper_first - lower_first)
        + drifts[1] * (upper_second - lower_second)
        + drifts[2] * (upper_third - lower_third)
    )
    first_shift, second_shift, third_shift = spectral_shifts
    real_part = centre[0]
    imag_part = centre[1]
    shifted = jnp.stack(
        [
            current_capacity * (first_shift * real_part - second_shift * imag_part),
            current_capacity * (second_shift * real_part + third_shift * imag_part),
        ]
    )
    return stencil + shifted


def inverse_diagonal(current_capacity, spectral_shifts, per_level_values):
    spread, _ = level_coefficients(per_level_values)
    first_shift, second_shift, third_shift = spectral_shifts
    top_left = current_capacity * first_shift + 6.0 * spread
    coupling = current_capacity * second_shift
    bottom_right = current_capacity * third_shift + 6.0 * spread
    determinant = top_left * bottom_right + coupling * coupling
    return (bottom_right / determinant, coupling / determinant, top_left / determinant)


def damped_update(residual_now, inverse):
    diagonal_a, diagonal_b, diagonal_c = inverse
    return OMEGA * jnp.stack(
        [
            diagonal_a * residual_now[0] + diagonal_b * residual_now[1],
            diagonal_c * residual_now[1] - diagonal_b * residual_now[0],
        ]
    )


def restrict_to_coarse(volume):
    leading = volume.shape[:-3]
    first_extent, second_extent, third_extent = volume.shape[-3:]
    blocks = volume.reshape(
        leading + (first_extent // 2, 2, second_extent // 2, 2, third_extent // 2, 2)
    )
    lead_count = len(leading)
    return jnp.mean(blocks, axis=(lead_count + 1, lead_count + 3, lead_count + 5))


def prolong_cells(volume):
    leading = volume.shape[:-3]
    first_extent, second_extent, third_extent = volume.shape[-3:]
    expanded = jnp.broadcast_to(
        volume[..., :, None, :, None, :, None],
        leading + (first_extent, 2, second_extent, 2, third_extent, 2),
    )
    return expanded.reshape(leading + (2 * first_extent, 2 * second_extent, 2 * third_extent))


def shift_values(frequency, length):
    ratio_step = ALPHA_CORNER ** (1.0 / length)
    phases = 2.0 * math.pi / length * frequency.astype(jnp.float32)
    first_shift = (1.0 - ratio_step * jnp.cos(phases)) / STEP_SIZE
    second_shift = ratio_step * jnp.sin(phases) / STEP_SIZE
    leading = frequency == 0
    second_shift = jnp.where(leading, 0.0, second_shift)
    third_shift = jnp.where(leading, (1.0 + ratio_step) / STEP_SIZE, first_shift)
    return tuple(
        (column.reshape(-1, 1, 1, 1) for column in (first_shift, second_shift, third_shift))
    )


def phase_grid(row_count, length):
    integers = (
        jnp.arange(row_count, dtype=jnp.int32)[:, None]
        * jnp.arange(length, dtype=jnp.int32)[None, :]
        % length
    )
    return 2.0 * math.pi / length * integers.astype(jnp.float32)


def pad_faces(volume):
    return extended(volume, (("space", 2),), 1)


def multigrid_cycle(
    per_level_values,
    forcing_term,
    capacity_fields,
    spectral_shifts,
    shared_values,
    assemble_level,
    assemble_parts,
):
    current_capacity = capacity_fields[per_level_values]
    inverse = inverse_diagonal(current_capacity, spectral_shifts, per_level_values)
    coarsest = per_level_values == GRID_DEPTH - 1
    current = damped_update(forcing_term, inverse)
    for _ in range((COARSE_SWEEPS if coarsest else SMOOTH) - 1):
        current = current + damped_update(
            forcing_term
            - apply_operator(
                pad_faces(current), current_capacity, spectral_shifts, per_level_values
            ),
            inverse,
        )
    if coarsest:
        return current
    coarse_right_hand = restrict_to_coarse(
        forcing_term
        - apply_operator(pad_faces(current), current_capacity, spectral_shifts, per_level_values)
    )
    coarse_solution = multigrid_cycle(
        per_level_values + 1,
        coarse_right_hand,
        capacity_fields,
        spectral_shifts,
        shared_values,
        assemble_level,
        assemble_parts,
    )
    current = current + prolong_cells(coarse_solution)
    for _ in range(SMOOTH):
        current = current + damped_update(
            forcing_term
            - apply_operator(
                pad_faces(current), current_capacity, spectral_shifts, per_level_values
            ),
            inverse,
        )
    return current


def slab_program(residual, capacity):
    steps_here, thickness, extent_second, extent_third = residual.shape
    length = lax.axis_size("tm") * steps_here
    ratio_step = ALPHA_CORNER ** (1.0 / length)
    moments = (lax.axis_index("tm") * steps_here + jnp.arange(steps_here, dtype=jnp.int32)).astype(
        jnp.float32
    )
    scaled = (residual * jnp.power(ratio_step, moments)[:, None, None, None]).reshape(
        steps_here, -1
    )
    series = lax.all_to_all(scaled, "tm", split_axis=1, concat_axis=0, tiled=True)
    all_weights = jnp.power(ratio_step, jnp.arange(length, dtype=jnp.float32))
    alternate = 1.0 - 2.0 * (jnp.arange(length, dtype=jnp.int32) % 2).astype(jnp.float32)
    capacity_fields = [capacity]
    for _ in range(1, GRID_DEPTH):
        capacity_fields.append(restrict_to_coarse(capacity_fields[-1]))
    halves = length // 2
    phases = phase_grid(halves, length)
    first_row = jnp.arange(halves, dtype=jnp.int32)[:, None] == 0
    forward = jnp.concatenate(
        [jnp.cos(phases), jnp.where(first_row, alternate[None, :], -jnp.sin(phases))], axis=0
    )
    spectrum = jnp.dot(forward, series, precision=HIGHEST).reshape(2, halves, -1)
    received = lax.all_to_all(spectrum, "tm", split_axis=1, concat_axis=2, tiled=True)
    slot_count = steps_here // 2
    frequency = lax.axis_index("tm") * slot_count + jnp.arange(slot_count, dtype=jnp.int32)
    spectral_shifts = shift_values(frequency, length)
    field_list = received.reshape(2, slot_count, thickness, extent_second, extent_third)
    solved_fields = multigrid_cycle(
        0, field_list, capacity_fields, spectral_shifts, False, GRID_DEPTH, None
    )
    flattened = solved_fields.reshape(2, slot_count, -1)
    returned = lax.all_to_all(flattened, "tm", split_axis=2, concat_axis=1, tiled=True)
    halves = length // 2
    phases = jnp.transpose(phase_grid(halves, length))
    first_column = jnp.arange(halves, dtype=jnp.int32)[None, :] == 0
    real_columns = jnp.where(first_column, 1.0, 2.0 * jnp.cos(phases)) / length
    imag_columns = jnp.where(first_column, alternate[:, None], -2.0 * jnp.sin(phases)) / length
    inverse_table = jnp.concatenate([real_columns, imag_columns], axis=1)
    values = jnp.dot(
        inverse_table,
        returned.reshape(returned.shape[0] * returned.shape[1], -1),
        precision=HIGHEST,
    )
    values = values / all_weights[:, None]
    result = lax.all_to_all(values, "tm", split_axis=0, concat_axis=1, tiled=True)
    return result.reshape(residual.shape)


def complex_add(p, q):
    return (p[0] + q[0], p[1] + q[1])


def complex_sub(p, q):
    return (p[0] - q[0], p[1] - q[1])


def complex_scale(p, cosine, sine):
    real, imag = p
    if abs(sine) < 1e-12:
        if abs(cosine - 1.0) < 1e-12:
            return p
        return (cosine * real, None if imag is None else cosine * imag)
    if imag is None:
        return (None if abs(cosine) < 1e-12 else cosine * real, sine * real)
    if abs(cosine) < 1e-12:
        if abs(sine - 1.0) < 1e-12:
            return (-imag, real)
        if abs(sine + 1.0) < 1e-12:
            return (imag, -real)
        return (-sine * imag, sine * real)
    return (cosine * real - sine * imag, cosine * imag + sine * real)


def full(p, like):
    return tuple(jnp.zeros_like(like) if part is None else part for part in p)


def transform(points, sign):
    count = len(points)
    if count == 1:
        return points
    if count % 2:
        sums = []
        for m in range(count):
            total = points[0]
            for s in range(1, count):
                angle = sign * 2.0 * math.pi * ((m * s) % count) / count
                term = complex_scale(points[s], math.cos(angle), math.sin(angle))
                total = complex_add(total, term)
            sums.append(total)
        return sums
    even = transform(points[0::2], sign)
    odd = transform(points[1::2], sign)
    low, high = [], []
    for m in range(count // 2):
        angle = sign * 2.0 * math.pi * m / count
        turned = complex_scale(odd[m], math.cos(angle), math.sin(angle))
        low.append(complex_add(even[m], turned))
        high.append(complex_sub(even[m], turned))
    return low + high


def pick(index, values):
    chosen = jnp.float32(values[-1])
    for place in range(len(values) - 1):
        chosen = jnp.where(index == place, jnp.float32(values[place]), chosen)
    return chosen


def forward_kernel(*refs):
    chunks, out = refs[:4], refs[4]
    steps, planes = chunks[0].shape[:2]
    length = 4 * steps
    ratio = ALPHA_CORNER ** (1.0 / length)
    me = lax.axis_index("tm")
    weights = []
    for m in range(4):
        block = jnp.bitwise_xor(me, m)
        grow = [ratio ** (steps * d) for d in range(4)]
        weights.append(
            (
                pick(block, grow),
                pick(block, [grow[0], -grow[1], grow[2], -grow[3]]),
                pick(block, [grow[0], 0.0, -grow[2], 0.0]),
                pick(block, [0.0, -grow[1], 0.0, grow[3]]),
            )
        )

    def column(j, carry):
        sums = [[], [], [], []]
        for s in range(steps):
            values = [chunk[s, j] for chunk in chunks]
            for kind in range(4):
                total = weights[0][kind] * values[0]
                for m in range(1, 4):
                    total = total + weights[m][kind] * values[m]
                sums[kind].append(total)

        def turned(real, imag, remainder):
            points = []
            for s in range(steps):
                angle = -2.0 * math.pi * remainder * s / length
                size = ratio**s
                point = (real[s], None if imag is None else imag[s])
                point = complex_scale(point, size * math.cos(angle), size * math.sin(angle))
                points.append(full(point, real[s]))
            return transform(points, -1.0)

        halves = length // 2
        found = {}
        for remainder, real, imag in ((0, sums[0], None), (2, sums[1], None), (1, sums[2], sums[3])):
            for m, value in enumerate(turned(real, imag, remainder)):
                slot = 4 * m + remainder
                if slot <= halves:
                    found[slot] = value
                elif remainder == 1:
                    found[length - slot] = (value[0], -value[1])
        out[0, 0, j] = found[0][0]
        out[0, 1, j] = found[halves][0]
        for slot in range(1, halves):
            out[slot, 0, j] = found[slot][0]
            out[slot, 1, j] = found[slot][1]
        return carry

    lax.fori_loop(0, planes, column, 0)


def backward_kernel(spectrum, *outs):
    steps, planes = outs[0].shape[:2]
    length = 4 * steps
    halves = length // 2
    ratio = ALPHA_CORNER ** (1.0 / length)
    me = lax.axis_index("tm")
    weights = []
    for m in range(4):
        block = jnp.bitwise_xor(me, m)
        grow = [ratio ** (-steps * d) / length for d in range(4)]
        weights.append(
            (
                pick(block, grow),
                pick(block, [grow[0], -grow[1], grow[2], -grow[3]]),
                pick(block, [2.0 * grow[0], 0.0, -2.0 * grow[2], 0.0]),
                pick(block, [0.0, -2.0 * grow[1], 0.0, 2.0 * grow[3]]),
            )
        )

    def column(j, carry):
        def value(slot):
            if slot == 0:
                return (spectrum[0, 0, j], jnp.zeros_like(spectrum[0, 0, j]))
            if slot == halves:
                return (spectrum[0, 1, j], jnp.zeros_like(spectrum[0, 1, j]))
            if slot < halves:
                return (spectrum[slot, 0, j], spectrum[slot, 1, j])
            return (spectrum[length - slot, 0, j], -spectrum[length - slot, 1, j])

        def turned(remainder):
            points = transform([value(4 * m + remainder) for m in range(steps)], 1.0)
            result = []
            for s in range(steps):
                angle = 2.0 * math.pi * remainder * s / length
                size = ratio**-s
                result.append(
                    complex_scale(points[s], size * math.cos(angle), size * math.sin(angle))
                )
            return result

        zero, two, one = turned(0), turned(2), turned(1)
        for s in range(steps):
            parts = (zero[s][0], two[s][0], one[s][0], one[s][1])
            for m in range(4):
                total = weights[m][0] * parts[0]
                for kind in range(1, 4):
                    total = total + weights[m][kind] * parts[kind]
                outs[m][s, j] = total
        return carry

    lax.fori_loop(0, planes, column, 0)


def split_kernel(residual, *refs):
    chunks, sems = refs[:-1], refs[-1]
    planes = chunks[0].shape[1]
    me = lax.axis_index("tm")
    copies = []
    for m, chunk in enumerate(chunks):
        block = jnp.bitwise_xor(me, m)
        source = residual.at[:, pl.ds(block * planes, planes)]
        copies.append(pltpu.make_async_copy(source, chunk, sems.at[m]))
        copies[-1].start()
    for copy in copies:
        copy.wait()


def place_kernel(*refs):
    chunks, out, sems = refs[:-2], refs[-2], refs[-1]
    planes = chunks[0].shape[1]
    me = lax.axis_index("tm")
    copies = []
    for m, chunk in enumerate(chunks):
        block = jnp.bitwise_xor(me, m)
        target = out.at[:, pl.ds(block * planes, planes)]
        copies.append(pltpu.make_async_copy(chunk, target, sems.at[m]))
        copies[-1].start()
    for copy in copies:
        copy.wait()


def cycle_kernel(blocks, forcing, out, *scratch, space_count, order):
    rows, lanes = forcing.shape[-2:]
    planes = forcing.shape[2]
    thickness = blocks.shape[1]
    slots = forcing.shape[0]
    length = 2 * slots
    ratio = ALPHA_CORNER ** (1.0 / length)
    me_space = lax.axis_index("space")
    slot = lax.axis_index("tm") * space_count + me_space
    angles = [2.0 * math.pi * k / length for k in range(slots)]
    first = [(1.0 - ratio * math.cos(a)) / STEP_SIZE for a in angles]
    second = [ratio * math.sin(a) / STEP_SIZE for a in angles]
    third = list(first)
    second[0] = 0.0
    third[0] = (1.0 + ratio) / STEP_SIZE
    first, second, third = (pick(slot, values) for values in (first, second, third))

    fields = [
        dict(zip(("capacity", "a", "b", "c", "u", "w", "g"), scratch[7 * l : 7 * l + 7]))
        for l in range(GRID_DEPTH)
    ]
    row = lax.broadcasted_iota(jnp.int32, (rows, lanes), 0)
    lane = lax.broadcasted_iota(jnp.int32, (rows, lanes), 1)

    for block, distance in enumerate(order):
        target = jnp.bitwise_xor(me_space, distance) * thickness
        for x in range(thickness):
            fields[0]["capacity"][target + x] = blocks[block, x]

    def loop(count, body):
        group = min(count, GROUP * thickness)
        assert count % group == 0 and (group % thickness == 0 or group == count)

        def step(i):
            for p in range(group):
                body(lambda unit: i * (group // unit), p)

        if count == group:
            step(0)
        else:
            lax.fori_loop(0, count // group, lambda i, carry: (step(i), carry)[1], 0)

    def pair_sum(value, level):
        stride = 2**level
        if stride < rows:
            bit = (row // stride) % 2 == 1
            value = value + jnp.where(
                bit, pltpu.roll(value, stride, 0), pltpu.roll(value, rows - stride, 0)
            )
        bit = (lane // stride) % 2 == 1
        return value + jnp.where(
            bit, pltpu.roll(value, stride, 1), pltpu.roll(value, lanes - stride, 1)
        )

    def level_count(level):
        return fields[level]["capacity"].shape[0]

    for level in range(1, GRID_DEPTH):
        fine, coarse = fields[level - 1]["capacity"], fields[level]["capacity"]

        def shrink(at, p, fine=fine, coarse=coarse, level=level):
            here = at(1) + p
            pair = fine[2 * here] + fine[2 * here + 1]
            coarse[here] = 0.125 * pair_sum(pair, level - 1)

        loop(level_count(level), shrink)

    def stencil(level):
        spread, drifts = level_coefficients(level)
        stride = 2**level
        extents = (rows // stride, lanes // stride)
        cell = (row // stride, lane // stride)
        masks = []
        for d in range(2):
            up = jnp.where(cell[d] < extents[d] - 1, spread - drifts[d + 1], 0.0)
            down = jnp.where(cell[d] > 0, spread + drifts[d + 1], 0.0)
            masks.append((up, down))

        def apply(here, up, down):
            total = (spread - drifts[0]) * up + (spread + drifts[0]) * down
            if extents[0] > 1:
                total = total + masks[0][0] * pltpu.roll(here, rows - stride, 0)
                total = total + masks[0][1] * pltpu.roll(here, stride, 0)
            total = total + masks[1][0] * pltpu.roll(here, lanes - stride, 1)
            return total + masks[1][1] * pltpu.roll(here, stride, 1)

        return apply

    def place(at, p):
        inner = p % thickness
        source = at(thickness) + p // thickness
        return (inner // planes) * space_count + source, inner % planes

    def forcing_at(level, at, p):
        if level:
            ref = fields[level]["g"]
            return ref[at(1) + p, 0], ref[at(1) + p, 1]
        index, inner = place(at, p)
        return forcing[index, 0, inner], forcing[index, 1, inner]

    def start(level):
        field = fields[level]
        spread, _ = level_coefficients(level)
        zero = jnp.zeros((rows, lanes), jnp.float32)
        for name in ("u", "w"):
            for edge in (0, level_count(level) + 1):
                field[name][edge, 0] = zero
                field[name][edge, 1] = zero

        def body(at, p):
            here = at(1) + p
            size = field["capacity"][here]
            top = size * first + 6.0 * spread
            couple = size * second
            bottom = size * third + 6.0 * spread
            inverse = OMEGA / (top * bottom + couple * couple)
            a, b, c = bottom * inverse, couple * inverse, top * inverse
            field["a"][here] = a
            field["b"][here] = b
            field["c"][here] = c
            real, imag = forcing_at(level, at, p)
            field["u"][here + 1, 0] = a * real + b * imag
            field["u"][here + 1, 1] = c * imag - b * real

        loop(level_count(level), body)

    def right_side(level, apply, source, at, p):
        here = at(1) + p
        real, imag = forcing_at(level, at, p)
        v_real, v_imag = source[here + 1, 0], source[here + 1, 1]
        r_real = real + apply(v_real, source[here + 2, 0], source[here, 0])
        r_imag = imag + apply(v_imag, source[here + 2, 1], source[here, 1])
        return v_real, v_imag, r_real, r_imag

    def sweep(level, source, store):
        field, apply = fields[level], stencil(level)

        def body(at, p):
            here = at(1) + p
            v_real, v_imag, r_real, r_imag = right_side(level, apply, source, at, p)
            a, b, c = field["a"][here], field["b"][here], field["c"][here]
            new_real = (1.0 - OMEGA) * v_real + (a * r_real + b * r_imag)
            new_imag = (1.0 - OMEGA) * v_imag + (c * r_imag - b * r_real)
            store(at, p, new_real, new_imag)

        loop(level_count(level), body)

    def storing(ref):
        def store(at, p, real, imag):
            ref[at(1) + p + 1, 0] = real
            ref[at(1) + p + 1, 1] = imag

        return store

    def store_out(at, p, real, imag):
        index, inner = place(at, p)
        out[index, 0, inner] = real
        out[index, 1, inner] = imag

    def descend(level, source):
        field, apply = fields[level], stencil(level)
        spread, _ = level_coefficients(level)
        coarse = fields[level + 1]["g"]

        def defect(at, p):
            here = at(1) + p
            v_real, v_imag, r_real, r_imag = right_side(level, apply, source, at, p)
            size = field["capacity"][here]
            real = r_real - 6.0 * spread * v_real - size * (first * v_real - second * v_imag)
            imag = r_imag - 6.0 * spread * v_imag - size * (second * v_real + third * v_imag)
            return real, imag

        def body(at, p):
            if p % 2:
                return
            low, high = defect(at, p), defect(at, p + 1)
            target = at(2) + p // 2
            for part in range(2):
                coarse[target, part] = 0.125 * pair_sum(low[part] + high[part], level)

        loop(level_count(level), body)

    def cycle(level, last_store):
        field = fields[level]
        here, other = field["u"], field["w"]
        start(level)
        coarsest = level == GRID_DEPTH - 1
        for _ in range((COARSE_SWEEPS if coarsest else SMOOTH) - 1):
            sweep(level, here, storing(other))
            here, other = other, here
        if coarsest:
            return here
        descend(level, here)
        value = cycle(level + 1, None)

        def correct(at, p, here=here, other=other):
            place = at(1) + p + 1
            for part in range(2):
                other[place, part] = here[place, part] + value[at(2) + p // 2 + 1, part]

        loop(level_count(level), correct)
        here, other = other, here
        for repeat in range(SMOOTH):
            final = repeat == SMOOTH - 1 and last_store is not None
            sweep(level, here, last_store if final else storing(other))
            here, other = other, here
        return here

    cycle(0, store_out)


def call(kernel, shapes, *operands, scratch=(), space_in=pltpu.VMEM, space_out=pltpu.VMEM):
    out_specs = jax.tree.map(lambda s: pl.BlockSpec(memory_space=space_out), shapes)
    return pl.pallas_call(
        kernel,
        out_shape=shapes,
        in_specs=[pl.BlockSpec(memory_space=space_in)] * len(operands),
        out_specs=out_specs,
        scratch_shapes=scratch,
        compiler_params=pltpu.CompilerParams(vmem_limit_bytes=VMEM_LIMIT),
    )(*operands)


def gather_capacity(capacity, space_count, chunks):
    blocks, strides = capacity[None], []
    order = [0]
    stride = 2
    while stride < space_count:
        strides.append(stride)
        stride *= 2
    strides.append(1)
    for stride in strides:
        if stride == 1:
            chunks[1:], blocks = lax.optimization_barrier((chunks[1:], blocks))
        pairs = [(k, k ^ stride) for k in range(space_count)]
        others = lax.ppermute(blocks, "space", pairs)
        blocks = jnp.concatenate([blocks, others], axis=0)
        order = order + [place ^ stride for place in order]
    return blocks, order


def run_cycle(blocks, spectrum, order):
    space_count, thickness, rows, lanes = blocks.shape
    scratch = []
    for level in range(GRID_DEPTH):
        count = (thickness * space_count) >> level
        scratch += [pltpu.VMEM((count, rows, lanes), jnp.float32)] * 4
        scratch += [pltpu.VMEM((count + 2, 2, rows, lanes), jnp.float32)] * 2
        small = level == 0
        scratch += [pltpu.VMEM((1 if small else count, 2, rows, lanes), jnp.float32)]
    return call(
        functools.partial(
            cycle_kernel, space_count=space_count, order=order
        ),
        jax.ShapeDtypeStruct(spectrum.shape, jnp.float32),
        blocks,
        spectrum,
        scratch=scratch,
    )


def slot_program(residual, capacity):
    steps, thickness, rows, lanes = residual.shape
    tm_count, space_count = lax.axis_size("tm"), lax.axis_size("space")
    slots = tm_count * space_count
    planes = thickness // tm_count
    chunk = jax.ShapeDtypeStruct((steps, planes, rows, lanes), jnp.float32)
    sems = [pltpu.SemaphoreType.DMA((tm_count,))]
    chunks = list(
        call(
            split_kernel,
            (chunk,) * tm_count,
            pltpu.with_memory_space_constraint(residual, pltpu.HBM),
            scratch=sems,
            space_in=pl.ANY,
        )
    )
    swaps = [[(k, k ^ m) for k in range(tm_count)] for m in range(tm_count)]
    for m in range(1, tm_count):
        chunks[m] = lax.ppermute(chunks[m], "tm", swaps[m])
    blocks, order = gather_capacity(capacity, space_count, chunks)
    spectrum = call(
        forward_kernel,
        pltpu.VMEM((slots, 2, planes, rows, lanes), jnp.float32),
        *chunks,
    )
    spectrum = lax.all_to_all(spectrum, ("tm", "space"), 0, 0, tiled=True)
    solved = run_cycle(blocks, spectrum, tuple(order))
    solved = lax.all_to_all(solved, ("tm", "space"), 0, 0, tiled=True)
    pieces = list(call(backward_kernel, (chunk,) * tm_count, solved))
    for m in range(1, tm_count):
        pieces[m] = lax.ppermute(pieces[m], "tm", swaps[m])
    whole = jax.ShapeDtypeStruct(residual.shape, jnp.float32)
    return call(place_kernel, whole, *pieces, scratch=sems, space_out=pl.ANY)


def on_device(residual, capacity):
    steps, thickness, _, _ = residual.shape
    tm_count, space_count = lax.axis_size("tm"), lax.axis_size("space")
    whole = (
        tm_count == 4
        and 2 * space_count == steps
        and space_count & (space_count - 1) == 0
        and space_count > 1
        and thickness % tm_count == 0
        and thickness % 2 == 0
    )
    if whole:
        return slot_program(residual, capacity)
    return slab_program(residual, capacity)


def solution(mesh):
    return jax.shard_map(
        on_device,
        mesh=mesh,
        in_specs=(P("tm", "space", None, None), P("space", None, None)),
        out_specs=P("tm", "space", None, None),
        check_vma=False,
    )
```

```python
import functools
import math

import jax
import jax.numpy as jnp
from jax import lax
from jax.experimental import pallas as pl
from jax.experimental.pallas import tpu as pltpu
from jax.sharding import PartitionSpec as P

GRID_DEPTH = 4
SMOOTH = 2
COARSE_SWEEPS = 6


ALPHA_CORNER = 0.01
STEP_SIZE = 0.5
DIFFUSE = 2.0
ADVECT = (0.2, -0.15, 0.1)
OMEGA = 0.7
HIGHEST = lax.Precision.HIGHEST
VMEM_LIMIT = 16 * 2**20
GROUP = 2


def extended(array, sides, width):
    for axis, dim in sides:
        peers, length = (lax.axis_size(axis), array.shape[dim])
        up = [(i, (i + 1) % peers) for i in range(peers - 1)]
        down = [(j, i) for i, j in up]
        last = lax.slice_in_dim(array, length - width, length, axis=dim)
        initial = lax.slice_in_dim(array, 0, width, axis=dim)
        before = lax.ppermute(last, axis, up)
        after = lax.ppermute(initial, axis, down)
        array = jnp.concatenate([before, array, after], axis=dim)
    return array


def level_coefficients(per_level_values):
    spread = DIFFUSE / 4.0**per_level_values
    drifts = tuple((component / 2.0**per_level_values for component in ADVECT))
    return (spread, drifts)


def pad_second(volume, position):
    widths = [(0, 0)] * volume.ndim
    widths[position] = (1, 1)
    return jnp.pad(volume, widths)


def apply_operator(padded, current_capacity, spectral_shifts, per_level_values):
    spread, drifts = level_coefficients(per_level_values)
    centre = padded[:, :, 1:-1]
    upper_first = padded[:, :, 2:]
    lower_first = padded[:, :, :-2]
    wide_second = pad_second(centre, 3)
    upper_second = wide_second[:, :, :, 2:]
    lower_second = wide_second[:, :, :, :-2]
    wide_third = pad_second(centre, 4)
    upper_third = wide_third[:, :, :, :, 2:]
    lower_third = wide_third[:, :, :, :, :-2]
    stencil = spread * (
        6.0 * centre
        - upper_first
        - lower_first
        - upper_second
        - lower_second
        - upper_third
        - lower_third
    )
    stencil = (
        stencil
        + drifts[0] * (upper_first - lower_first)
        + drifts[1] * (upper_second - lower_second)
        + drifts[2] * (upper_third - lower_third)
    )
    first_shift, second_shift, third_shift = spectral_shifts
    real_part = centre[0]
    imag_part = centre[1]
    shifted = jnp.stack(
        [
            current_capacity * (first_shift * real_part - second_shift * imag_part),
            current_capacity * (second_shift * real_part + third_shift * imag_part),
        ]
    )
    return stencil + shifted


def inverse_diagonal(current_capacity, spectral_shifts, per_level_values):
    spread, _ = level_coefficients(per_level_values)
    first_shift, second_shift, third_shift = spectral_shifts
    top_left = current_capacity * first_shift + 6.0 * spread
    coupling = current_capacity * second_shift
    bottom_right = current_capacity * third_shift + 6.0 * spread
    determinant = top_left * bottom_right + coupling * coupling
    return (bottom_right / determinant, coupling / determinant, top_left / determinant)


def damped_update(residual_now, inverse):
    diagonal_a, diagonal_b, diagonal_c = inverse
    return OMEGA * jnp.stack(
        [
            diagonal_a * residual_now[0] + diagonal_b * residual_now[1],
            diagonal_c * residual_now[1] - diagonal_b * residual_now[0],
        ]
    )


def restrict_to_coarse(volume):
    leading = volume.shape[:-3]
    first_extent, second_extent, third_extent = volume.shape[-3:]
    blocks = volume.reshape(
        leading + (first_extent // 2, 2, second_extent // 2, 2, third_extent // 2, 2)
    )
    lead_count = len(leading)
    return jnp.mean(blocks, axis=(lead_count + 1, lead_count + 3, lead_count + 5))


def prolong_cells(volume):
    leading = volume.shape[:-3]
    first_extent, second_extent, third_extent = volume.shape[-3:]
    expanded = jnp.broadcast_to(
        volume[..., :, None, :, None, :, None],
        leading + (first_extent, 2, second_extent, 2, third_extent, 2),
    )
    return expanded.reshape(leading + (2 * first_extent, 2 * second_extent, 2 * third_extent))


def shift_values(frequency, length):
    ratio_step = ALPHA_CORNER ** (1.0 / length)
    phases = 2.0 * math.pi / length * frequency.astype(jnp.float32)
    first_shift = (1.0 - ratio_step * jnp.cos(phases)) / STEP_SIZE
    second_shift = ratio_step * jnp.sin(phases) / STEP_SIZE
    leading = frequency == 0
    second_shift = jnp.where(leading, 0.0, second_shift)
    third_shift = jnp.where(leading, (1.0 + ratio_step) / STEP_SIZE, first_shift)
    return tuple(
        (column.reshape(-1, 1, 1, 1) for column in (first_shift, second_shift, third_shift))
    )


def phase_grid(row_count, length):
    integers = (
        jnp.arange(row_count, dtype=jnp.int32)[:, None]
        * jnp.arange(length, dtype=jnp.int32)[None, :]
        % length
    )
    return 2.0 * math.pi / length * integers.astype(jnp.float32)


def pad_faces(volume):
    return extended(volume, (("space", 2),), 1)


def multigrid_cycle(
    per_level_values,
    forcing_term,
    capacity_fields,
    spectral_shifts,
    shared_values,
    assemble_level,
    assemble_parts,
):
    current_capacity = capacity_fields[per_level_values]
    inverse = inverse_diagonal(current_capacity, spectral_shifts, per_level_values)
    coarsest = per_level_values == GRID_DEPTH - 1
    current = damped_update(forcing_term, inverse)
    for _ in range((COARSE_SWEEPS if coarsest else SMOOTH) - 1):
        current = current + damped_update(
            forcing_term
            - apply_operator(
                pad_faces(current), current_capacity, spectral_shifts, per_level_values
            ),
            inverse,
        )
    if coarsest:
        return current
    coarse_right_hand = restrict_to_coarse(
        forcing_term
        - apply_operator(pad_faces(current), current_capacity, spectral_shifts, per_level_values)
    )
    coarse_solution = multigrid_cycle(
        per_level_values + 1,
        coarse_right_hand,
        capacity_fields,
        spectral_shifts,
        shared_values,
        assemble_level,
        assemble_parts,
    )
    current = current + prolong_cells(coarse_solution)
    for _ in range(SMOOTH):
        current = current + damped_update(
            forcing_term
            - apply_operator(
                pad_faces(current), current_capacity, spectral_shifts, per_level_values
            ),
            inverse,
        )
    return current


def slab_program(residual, capacity):
    steps_here, thickness, extent_second, extent_third = residual.shape
    length = lax.axis_size("tm") * steps_here
    ratio_step = ALPHA_CORNER ** (1.0 / length)
    moments = (lax.axis_index("tm") * steps_here + jnp.arange(steps_here, dtype=jnp.int32)).astype(
        jnp.float32
    )
    scaled = (residual * jnp.power(ratio_step, moments)[:, None, None, None]).reshape(
        steps_here, -1
    )
    series = lax.all_to_all(scaled, "tm", split_axis=1, concat_axis=0, tiled=True)
    all_weights = jnp.power(ratio_step, jnp.arange(length, dtype=jnp.float32))
    alternate = 1.0 - 2.0 * (jnp.arange(length, dtype=jnp.int32) % 2).astype(jnp.float32)
    capacity_fields = [capacity]
    for _ in range(1, GRID_DEPTH):
        capacity_fields.append(restrict_to_coarse(capacity_fields[-1]))
    halves = length // 2
    phases = phase_grid(halves, length)
    first_row = jnp.arange(halves, dtype=jnp.int32)[:, None] == 0
    forward = jnp.concatenate(
        [jnp.cos(phases), jnp.where(first_row, alternate[None, :], -jnp.sin(phases))], axis=0
    )
    spectrum = jnp.dot(forward, series, precision=HIGHEST).reshape(2, halves, -1)
    received = lax.all_to_all(spectrum, "tm", split_axis=1, concat_axis=2, tiled=True)
    slot_count = steps_here // 2
    frequency = lax.axis_index("tm") * slot_count + jnp.arange(slot_count, dtype=jnp.int32)
    spectral_shifts = shift_values(frequency, length)
    field_list = received.reshape(2, slot_count, thickness, extent_second, extent_third)
    solved_fields = multigrid_cycle(
        0, field_list, capacity_fields, spectral_shifts, False, GRID_DEPTH, None
    )
    flattened = solved_fields.reshape(2, slot_count, -1)
    returned = lax.all_to_all(flattened, "tm", split_axis=2, concat_axis=1, tiled=True)
    halves = length // 2
    phases = jnp.transpose(phase_grid(halves, length))
    first_column = jnp.arange(halves, dtype=jnp.int32)[None, :] == 0
    real_columns = jnp.where(first_column, 1.0, 2.0 * jnp.cos(phases)) / length
    imag_columns = jnp.where(first_column, alternate[:, None], -2.0 * jnp.sin(phases)) / length
    inverse_table = jnp.concatenate([real_columns, imag_columns], axis=1)
    values = jnp.dot(
        inverse_table,
        returned.reshape(returned.shape[0] * returned.shape[1], -1),
        precision=HIGHEST,
    )
    values = values / all_weights[:, None]
    result = lax.all_to_all(values, "tm", split_axis=0, concat_axis=1, tiled=True)
    return result.reshape(residual.shape)


def complex_add(p, q):
    return (p[0] + q[0], p[1] + q[1])


def complex_sub(p, q):
    return (p[0] - q[0], p[1] - q[1])


def complex_scale(p, cosine, sine):
    real, imag = p
    if abs(sine) < 1e-12:
        if abs(cosine - 1.0) < 1e-12:
            return p
        return (cosine * real, None if imag is None else cosine * imag)
    if imag is None:
        return (None if abs(cosine) < 1e-12 else cosine * real, sine * real)
    if abs(cosine) < 1e-12:
        if abs(sine - 1.0) < 1e-12:
            return (-imag, real)
        if abs(sine + 1.0) < 1e-12:
            return (imag, -real)
        return (-sine * imag, sine * real)
    return (cosine * real - sine * imag, cosine * imag + sine * real)


def full(p, like):
    return tuple(jnp.zeros_like(like) if part is None else part for part in p)


def transform(points, sign):
    count = len(points)
    if count == 1:
        return points
    if count % 2:
        sums = []
        for m in range(count):
            total = points[0]
            for s in range(1, count):
                angle = sign * 2.0 * math.pi * ((m * s) % count) / count
                term = complex_scale(points[s], math.cos(angle), math.sin(angle))
                total = complex_add(total, term)
            sums.append(total)
        return sums
    even = transform(points[0::2], sign)
    odd = transform(points[1::2], sign)
    low, high = [], []
    for m in range(count // 2):
        angle = sign * 2.0 * math.pi * m / count
        turned = complex_scale(odd[m], math.cos(angle), math.sin(angle))
        low.append(complex_add(even[m], turned))
        high.append(complex_sub(even[m], turned))
    return low + high


def pick(index, values):
    chosen = jnp.float32(values[-1])
    for place in range(len(values) - 1):
        chosen = jnp.where(index == place, jnp.float32(values[place]), chosen)
    return chosen


def forward_kernel(*refs):
    chunks, out = refs[:4], refs[4]
    steps, planes = chunks[0].shape[:2]
    length = 4 * steps
    ratio = ALPHA_CORNER ** (1.0 / length)
    me = lax.axis_index("tm")
    weights = []
    for m in range(4):
        block = jnp.bitwise_xor(me, m)
        grow = [ratio ** (steps * d) for d in range(4)]
        weights.append(
            (
                pick(block, grow),
                pick(block, [grow[0], -grow[1], grow[2], -grow[3]]),
                pick(block, [grow[0], 0.0, -grow[2], 0.0]),
                pick(block, [0.0, -grow[1], 0.0, grow[3]]),
            )
        )

    def column(j, carry):
        sums = [[], [], [], []]
        for s in range(steps):
            values = [chunk[s, j] for chunk in chunks]
            for kind in range(4):
                total = weights[0][kind] * values[0]
                for m in range(1, 4):
                    total = total + weights[m][kind] * values[m]
                sums[kind].append(total)

        def turned(real, imag, remainder):
            points = []
            for s in range(steps):
                angle = -2.0 * math.pi * remainder * s / length
                size = ratio**s
                point = (real[s], None if imag is None else imag[s])
                point = complex_scale(point, size * math.cos(angle), size * math.sin(angle))
                points.append(full(point, real[s]))
            return transform(points, -1.0)

        halves = length // 2
        found = {}
        for remainder, real, imag in ((0, sums[0], None), (2, sums[1], None), (1, sums[2], sums[3])):
            for m, value in enumerate(turned(real, imag, remainder)):
                slot = 4 * m + remainder
                if slot <= halves:
                    found[slot] = value
                elif remainder == 1:
                    found[length - slot] = (value[0], -value[1])
        out[0, 0, j] = found[0][0]
        out[0, 1, j] = found[halves][0]
        for slot in range(1, halves):
            out[slot, 0, j] = found[slot][0]
            out[slot, 1, j] = found[slot][1]
        return carry

    lax.fori_loop(0, planes, column, 0)


def backward_kernel(spectrum, *outs):
    steps, planes = outs[0].shape[:2]
    length = 4 * steps
    halves = length // 2
    ratio = ALPHA_CORNER ** (1.0 / length)
    me = lax.axis_index("tm")
    weights = []
    for m in range(4):
        block = jnp.bitwise_xor(me, m)
        grow = [ratio ** (-steps * d) / length for d in range(4)]
        weights.append(
            (
                pick(block, grow),
                pick(block, [grow[0], -grow[1], grow[2], -grow[3]]),
                pick(block, [2.0 * grow[0], 0.0, -2.0 * grow[2], 0.0]),
                pick(block, [0.0, -2.0 * grow[1], 0.0, 2.0 * grow[3]]),
            )
        )

    def column(j, carry):
        def value(slot):
            if slot == 0:
                return (spectrum[0, 0, j], jnp.zeros_like(spectrum[0, 0, j]))
            if slot == halves:
                return (spectrum[0, 1, j], jnp.zeros_like(spectrum[0, 1, j]))
            if slot < halves:
                return (spectrum[slot, 0, j], spectrum[slot, 1, j])
            return (spectrum[length - slot, 0, j], -spectrum[length - slot, 1, j])

        def turned(remainder):
            points = transform([value(4 * m + remainder) for m in range(steps)], 1.0)
            result = []
            for s in range(steps):
                angle = 2.0 * math.pi * remainder * s / length
                size = ratio**-s
                result.append(
                    complex_scale(points[s], size * math.cos(angle), size * math.sin(angle))
                )
            return result

        zero, two, one = turned(0), turned(2), turned(1)
        for s in range(steps):
            parts = (zero[s][0], two[s][0], one[s][0], one[s][1])
            for m in range(4):
                total = weights[m][0] * parts[0]
                for kind in range(1, 4):
                    total = total + weights[m][kind] * parts[kind]
                outs[m][s, j] = total
        return carry

    lax.fori_loop(0, planes, column, 0)


def split_kernel(residual, *refs, swaps):
    chunks, sems = refs[:-1], refs[-1]
    planes = chunks[0].shape[1]
    me = lax.axis_index("tm")
    copies = []
    for m, chunk in zip(swaps, chunks):
        block = jnp.bitwise_xor(me, m)
        source = residual.at[:, pl.ds(block * planes, planes)]
        copies.append(pltpu.make_async_copy(source, chunk, sems.at[m]))
        copies[-1].start()
    for copy in copies:
        copy.wait()


def place_kernel(*refs, swaps):
    chunks, out, sems = refs[: len(swaps)], refs[-2], refs[-1]
    planes = chunks[0].shape[1]
    me = lax.axis_index("tm")
    copies = []
    for m, chunk in zip(swaps, chunks):
        block = jnp.bitwise_xor(me, m)
        target = out.at[:, pl.ds(block * planes, planes)]
        copies.append(pltpu.make_async_copy(chunk, target, sems.at[m]))
        copies[-1].start()
    for copy in copies:
        copy.wait()


def cycle_kernel(*refs, space_count, order):
    parts, (forcing, out), scratch = refs[: len(order)], refs[len(order) :][:2], refs[len(order) + 2 :]
    rows, lanes = forcing.shape[-2:]
    planes = forcing.shape[2]
    thickness = parts[0].shape[1]
    slots = forcing.shape[0]
    length = 2 * slots
    ratio = ALPHA_CORNER ** (1.0 / length)
    me_space = lax.axis_index("space")
    slot = lax.axis_index("tm") * space_count + me_space
    angles = [2.0 * math.pi * k / length for k in range(slots)]
    first = [(1.0 - ratio * math.cos(a)) / STEP_SIZE for a in angles]
    second = [ratio * math.sin(a) / STEP_SIZE for a in angles]
    third = list(first)
    second[0] = 0.0
    third[0] = (1.0 + ratio) / STEP_SIZE
    first, second, third = (pick(slot, values) for values in (first, second, third))

    fields = [
        dict(zip(("capacity", "a", "b", "c", "u", "w", "g"), scratch[7 * l : 7 * l + 7]))
        for l in range(GRID_DEPTH)
    ]
    row = lax.broadcasted_iota(jnp.int32, (rows, lanes), 0)
    lane = lax.broadcasted_iota(jnp.int32, (rows, lanes), 1)

    for part, distances in zip(parts, order):
        for block, distance in enumerate(distances):
            target = jnp.bitwise_xor(me_space, distance) * thickness
            for x in range(thickness):
                fields[0]["capacity"][target + x] = part[block, x]

    def loop(count, body):
        group = min(count, GROUP * thickness)
        assert count % group == 0 and (group % thickness == 0 or group == count)

        def step(i):
            for p in range(group):
                body(lambda unit: i * (group // unit), p)

        if count == group:
            step(0)
        else:
            lax.fori_loop(0, count // group, lambda i, carry: (step(i), carry)[1], 0)

    def pair_sum(value, level):
        stride = 2**level
        if stride < rows:
            bit = (row // stride) % 2 == 1
            value = value + jnp.where(
                bit, pltpu.roll(value, stride, 0), pltpu.roll(value, rows - stride, 0)
            )
        bit = (lane // stride) % 2 == 1
        return value + jnp.where(
            bit, pltpu.roll(value, stride, 1), pltpu.roll(value, lanes - stride, 1)
        )

    def level_count(level):
        return fields[level]["capacity"].shape[0]

    for level in range(1, GRID_DEPTH):
        fine, coarse = fields[level - 1]["capacity"], fields[level]["capacity"]

        def shrink(at, p, fine=fine, coarse=coarse, level=level):
            here = at(1) + p
            pair = fine[2 * here] + fine[2 * here + 1]
            coarse[here] = 0.125 * pair_sum(pair, level - 1)

        loop(level_count(level), shrink)

    def stencil(level):
        spread, drifts = level_coefficients(level)
        stride = 2**level
        extents = (rows // stride, lanes // stride)
        cell = (row // stride, lane // stride)
        masks = []
        for d in range(2):
            up = jnp.where(cell[d] < extents[d] - 1, spread - drifts[d + 1], 0.0)
            down = jnp.where(cell[d] > 0, spread + drifts[d + 1], 0.0)
            masks.append((up, down))

        def apply(here, up, down):
            total = (spread - drifts[0]) * up + (spread + drifts[0]) * down
            if extents[0] > 1:
                total = total + masks[0][0] * pltpu.roll(here, rows - stride, 0)
                total = total + masks[0][1] * pltpu.roll(here, stride, 0)
            total = total + masks[1][0] * pltpu.roll(here, lanes - stride, 1)
            return total + masks[1][1] * pltpu.roll(here, stride, 1)

        return apply

    def place(at, p):
        inner = p % thickness
        source = at(thickness) + p // thickness
        return (inner // planes) * space_count + source, inner % planes

    def forcing_at(level, at, p):
        if level:
            ref = fields[level]["g"]
            return ref[at(1) + p, 0], ref[at(1) + p, 1]
        index, inner = place(at, p)
        return forcing[index, 0, inner], forcing[index, 1, inner]

    def start(level):
        field = fields[level]
        spread, _ = level_coefficients(level)
        zero = jnp.zeros((rows, lanes), jnp.float32)
        for name in ("u", "w"):
            for edge in (0, level_count(level) + 1):
                field[name][edge, 0] = zero
                field[name][edge, 1] = zero

        def body(at, p):
            here = at(1) + p
            size = field["capacity"][here]
            top = size * first + 6.0 * spread
            couple = size * second
            bottom = size * third + 6.0 * spread
            inverse = OMEGA / (top * bottom + couple * couple)
            a, b, c = bottom * inverse, couple * inverse, top * inverse
            field["a"][here] = a
            field["b"][here] = b
            field["c"][here] = c
            real, imag = forcing_at(level, at, p)
            field["u"][here + 1, 0] = a * real + b * imag
            field["u"][here + 1, 1] = c * imag - b * real

        loop(level_count(level), body)

    def right_side(level, apply, source, at, p):
        here = at(1) + p
        real, imag = forcing_at(level, at, p)
        v_real, v_imag = source[here + 1, 0], source[here + 1, 1]
        r_real = real + apply(v_real, source[here + 2, 0], source[here, 0])
        r_imag = imag + apply(v_imag, source[here + 2, 1], source[here, 1])
        return v_real, v_imag, r_real, r_imag

    def sweep(level, source, store):
        field, apply = fields[level], stencil(level)

        def body(at, p):
            here = at(1) + p
            v_real, v_imag, r_real, r_imag = right_side(level, apply, source, at, p)
            a, b, c = field["a"][here], field["b"][here], field["c"][here]
            new_real = (1.0 - OMEGA) * v_real + (a * r_real + b * r_imag)
            new_imag = (1.0 - OMEGA) * v_imag + (c * r_imag - b * r_real)
            store(at, p, new_real, new_imag)

        loop(level_count(level), body)

    def storing(ref):
        def store(at, p, real, imag):
            ref[at(1) + p + 1, 0] = real
            ref[at(1) + p + 1, 1] = imag

        return store

    def store_out(at, p, real, imag):
        index, inner = place(at, p)
        out[index, 0, inner] = real
        out[index, 1, inner] = imag

    def descend(level, source):
        field, apply = fields[level], stencil(level)
        spread, _ = level_coefficients(level)
        coarse = fields[level + 1]["g"]

        def defect(at, p):
            here = at(1) + p
            v_real, v_imag, r_real, r_imag = right_side(level, apply, source, at, p)
            size = field["capacity"][here]
            real = r_real - 6.0 * spread * v_real - size * (first * v_real - second * v_imag)
            imag = r_imag - 6.0 * spread * v_imag - size * (second * v_real + third * v_imag)
            return real, imag

        def body(at, p):
            if p % 2:
                return
            low, high = defect(at, p), defect(at, p + 1)
            target = at(2) + p // 2
            for part in range(2):
                coarse[target, part] = 0.125 * pair_sum(low[part] + high[part], level)

        loop(level_count(level), body)

    def cycle(level, last_store):
        field = fields[level]
        here, other = field["u"], field["w"]
        start(level)
        coarsest = level == GRID_DEPTH - 1
        for _ in range((COARSE_SWEEPS if coarsest else SMOOTH) - 1):
            sweep(level, here, storing(other))
            here, other = other, here
        if coarsest:
            return here
        descend(level, here)
        value = cycle(level + 1, None)

        def correct(at, p, here=here, other=other):
            place = at(1) + p + 1
            for part in range(2):
                other[place, part] = here[place, part] + value[at(2) + p // 2 + 1, part]

        loop(level_count(level), correct)
        here, other = other, here
        for repeat in range(SMOOTH):
            final = repeat == SMOOTH - 1 and last_store is not None
            sweep(level, here, last_store if final else storing(other))
            here, other = other, here
        return here

    cycle(0, store_out)


def arrived_kernel(array, same):
    pass


def call(
    kernel, shapes, *operands, scratch=(), space_in=pltpu.VMEM, space_out=pltpu.VMEM, aliases=None
):
    out_specs = jax.tree.map(lambda s: pl.BlockSpec(memory_space=space_out), shapes)
    return pl.pallas_call(
        kernel,
        out_shape=shapes,
        in_specs=[pl.BlockSpec(memory_space=space_in)] * len(operands),
        out_specs=out_specs,
        scratch_shapes=scratch,
        input_output_aliases=aliases or {},
        compiler_params=pltpu.CompilerParams(vmem_limit_bytes=VMEM_LIMIT),
    )(*operands)


def run_cycle(parts, spectrum, order, space_count):
    thickness, rows, lanes = parts[0].shape[1:]
    scratch = []
    for level in range(GRID_DEPTH):
        count = (thickness * space_count) >> level
        scratch += [pltpu.VMEM((count, rows, lanes), jnp.float32)] * 4
        scratch += [pltpu.VMEM((count + 2, 2, rows, lanes), jnp.float32)] * 2
        small = level == 0
        scratch += [pltpu.VMEM((1 if small else count, 2, rows, lanes), jnp.float32)]
    return call(
        functools.partial(cycle_kernel, space_count=space_count, order=order),
        jax.ShapeDtypeStruct(spectrum.shape, jnp.float32),
        *parts,
        spectrum,
        scratch=scratch,
    )


def exchanged(array, axis, distance):
    pairs = [(k, k ^ distance) for k in range(lax.axis_size(axis))]
    return lax.ppermute(array, axis, pairs)


def gather_capacity(capacity, space_count):
    parts, order = [capacity[None]], [(0,)]
    strides = [1 << k for k in range(1, space_count.bit_length() - 1)]
    strides[1:1] = [1]
    for stride in strides:
        if len(parts) > 1:
            parts, order = [jnp.concatenate(parts, axis=0)], [sum(order, ())]
        parts.append(exchanged(parts[0], "space", stride))
        order.append(tuple(place ^ stride for place in order[0]))
    return parts, tuple(order)


def slot_program(residual, capacity):
    steps, thickness, rows, lanes = residual.shape
    tm_count, space_count = lax.axis_size("tm"), lax.axis_size("space")
    slots = tm_count * space_count
    planes = thickness // tm_count
    chunk = jax.ShapeDtypeStruct((steps, planes, rows, lanes), jnp.float32)
    sems = [pltpu.SemaphoreType.DMA((tm_count,))]
    source = pltpu.with_memory_space_constraint(residual, pltpu.HBM)
    chunks = list(
        call(
            functools.partial(split_kernel, swaps=range(tm_count)),
            (chunk,) * tm_count,
            source,
            scratch=sems,
            space_in=pl.ANY,
        )
    )
    for m in range(1, tm_count):
        chunks[m] = exchanged(chunks[m], "tm", m)
    parts, order = gather_capacity(capacity, space_count)
    spectrum = call(
        forward_kernel,
        jax.ShapeDtypeStruct((slots, 2, planes, rows, lanes), jnp.float32),
        *chunks,
    )
    spectrum = lax.all_to_all(spectrum, ("tm", "space"), 0, 0, tiled=True)
    spectrum = call(
        arrived_kernel,
        jax.ShapeDtypeStruct(spectrum.shape, jnp.float32),
        spectrum,
        space_in=pl.ANY,
        space_out=pl.ANY,
        aliases={0: 0},
    )
    solved = run_cycle(parts, spectrum, order, space_count)
    solved = lax.all_to_all(solved, ("tm", "space"), 0, 0, tiled=True)
    pieces = list(call(backward_kernel, (chunk,) * tm_count, solved))
    for m in range(1, tm_count):
        pieces[m] = exchanged(pieces[m], "tm", m)
    whole = jax.ShapeDtypeStruct(residual.shape, jnp.float32)
    result = ()
    for swaps in ((0, 1, 2), (3,)):
        result = call(
            functools.partial(place_kernel, swaps=swaps),
            whole,
            *[pieces[m] for m in swaps],
            *result,
            scratch=sems,
            space_in=pl.ANY,
            space_out=pl.ANY,
            aliases={len(swaps): 0} if result else None,
        )
        result = (result,)
    return result[0]


def on_device(residual, capacity):
    steps, thickness, _, _ = residual.shape
    tm_count, space_count = lax.axis_size("tm"), lax.axis_size("space")
    whole = (
        tm_count == 4
        and 2 * space_count == steps
        and space_count & (space_count - 1) == 0
        and space_count > 1
        and thickness % tm_count == 0
        and thickness % 2 == 0
    )
    if whole:
        return slot_program(residual, capacity)
    return slab_program(residual, capacity)


def solution(mesh):
    return jax.shard_map(
        on_device,
        mesh=mesh,
        in_specs=(P("tm", "space", None, None), P("space", None, None)),
        out_specs=P("tm", "space", None, None),
        check_vma=False,
    )
```
